32 devices in a mesh: ta: 4 (over y, x), gz: 2 (over core), xy: 4 (over z).
Axes of the slice: x: 2, y: 2, z: 4, core: 2. Of those that a mesh axis runs over, the one named last changes fastest.
Arguments:
- source_field: float32 [2, 4, 3, 4, 2, 4, 128], P(None, None, None, 'ta', 'gz', 'xy'), may hold values from -6 to 6
- gauge_links: float32 [2, 8, 3, 3, 4, 2, 4, 128], P(None, None, None, None, 'ta', 'gz', 'xy'), may hold values from -2.5 to 2.5
- fine_vectors: bfloat16 [2, 24, 4, 3, 4, 2, 4, 128], P(None, None, None, None, 'ta', 'gz', 'xy'), may hold values from -1.75 to 1.75
- middle_blocks: float32 [2, 9, 24, 4, 2, 4, 768], P(None, None, None, 'ta', 'gz', 'xy'), may hold values from -0.3125 to 0.3125
- middle_vectors: float32 [2, 24, 4, 2, 4, 768], P(None, None, 'ta', 'gz', 'xy'), may hold values from -0.625 to 0.625
- bottom_blocks: float32 [2, 7, 4, 2, 2304], P(None, None, 'ta', 'gz'), may hold values from -4 to 4
Outputs:
- solution: float32 [2, 4, 3, 4, 2, 4, 128], P(None, None, None, 'ta', 'gz', 'xy')
- smoothed_residual: float32 [2, 4, 3, 4, 2, 4, 128], P(None, None, None, 'ta', 'gz', 'xy')
The draws below stay inside these ranges and needn't reach their ends.
All inputs are finite; a program needn't handle non-finite values.
Results may differ from the reference program's by a relative error of at most 0.0034.
Values sent between devices are 32-bit elements; how exact they have to be, the bound alone decides.
A program may use at most 64 MiB of HBM per device.

```python
import math
import jax
import jax.numpy as jnp
import numpy as np
from jax import lax

TL = 1
ZL = 1
XL = 1
YL = 128
BY = 4
NVEC = 24
NVEC2 = 24
YBLOCKS = 32
NT = 4
NZ = 2
NX = 4
N_TA = 4
N_GZ = 2
N_XY = 4


def draw_bottom_blocks(key, part):
    shape_list = (2, 7, NVEC2, NVEC2, N_TA, N_GZ, N_XY)
    entries = jax.random.normal(jax.random.fold_in(key, 11), shape_list, jnp.float32)
    spread = jnp.exp(jax.random.uniform(jax.random.fold_in(key, 13), (N_TA, N_GZ, N_XY), jnp.float32, -1.2, 1.2))
    rising = 3.0 ** (jnp.arange(N_TA, dtype=jnp.float32) / max(N_TA - 1, 1))
    scaling = spread * rising[:, None, None] / math.sqrt(14.0 * NVEC2)
    blocks = jnp.clip(entries * scaling, -4.0, 4.0)
    ordered = jnp.transpose(blocks, (0, 1, 4, 5, 6, 2, 3))
    return ordered.reshape((2, 7, N_TA, N_GZ, N_XY * NVEC2 * NVEC2))


def level_of(stream_key, dims, cuts, smallest, top_value):
    loudness, own = 1.0, jax.random.fold_in(stream_key, 6)
    for position, shards_of in cuts:
        draws = jnp.exp(jax.random.uniform(jax.random.fold_in(own, position), (shards_of,), jnp.float32, smallest / len(cuts), top_value / len(cuts)))
        loudness = loudness * jnp.repeat(draws, dims[position] // shards_of).reshape([-1 if axis == position else 1 for axis in range(len(dims))])
    return loudness


def bell_draw(own_key, dims, scale, limit, pieces=(), kind=jnp.bfloat16):
    level = level_of(own_key, dims, pieces, -0.22, 0.18) if pieces else 1.0
    drawn = jax.random.normal(own_key, dims, jnp.float32) * scale * level
    return jnp.minimum(jnp.maximum(drawn, -limit), limit).astype(kind)


def setup_inputs(seed: int = 0) -> dict:
    seeds = jax.random.split(jax.random.key(seed), 7)
    return {
        "source_field": bell_draw(seeds[0], (2, 4, 3, NT, NZ, NX, YL), 1.0, 6.0, ((3, 4), (4, 2), (5, 4)), jnp.float32),
        "gauge_links": bell_draw(seeds[1], (2, 8, 3, 3, NT, NZ, NX, YL), 6 ** -0.5, 2.5, ((4, 4), (5, 2), (6, 4)), jnp.float32),
        "fine_vectors": bell_draw(seeds[2], (2, NVEC, 4, 3, NT, NZ, NX, YL), (TL * ZL * XL * BY * 3) ** -0.5, 1.75, ((4, 4), (5, 2), (6, 4))),
        "middle_blocks": bell_draw(seeds[3], (2, 9, NVEC, N_TA, N_GZ, N_XY, NVEC * YBLOCKS), (18 * NVEC) ** -0.5, 0.3125, ((3, 4), (4, 2), (5, 4)), jnp.float32),
        "middle_vectors": bell_draw(seeds[4], (2, NVEC2, N_TA, N_GZ, N_XY, NVEC * YBLOCKS), (4 * NVEC) ** -0.5, 0.625, ((2, 4), (3, 2), (4, 4)), jnp.float32),
        "bottom_blocks": draw_bottom_blocks(jax.random.fold_in(seeds[6], 71), 0),
    }


quark_mass = 0.1
twist_mass = 0.1
fine_damping = 0.8
middle_damping = 0.4
middle_shift = 2.0
bottom_shift = 2.0

gamma_real = np.array([
    [[0, 0, 1, 0], [0, 0, 0, 1], [1, 0, 0, 0], [0, 1, 0, 0]],
    [[0] * 4] * 4,
    [[0] * 4] * 4,
    [[0, 0, 0, -1], [0, 0, 1, 0], [0, 1, 0, 0], [-1, 0, 0, 0]]], np.float32)
gamma_imag = np.array([
    [[0] * 4] * 4,
    [[0, 0, 1, 0], [0, 0, 0, -1], [-1, 0, 0, 0], [0, 1, 0, 0]],
    [[0, 0, 0, 1], [0, 0, 1, 0], [0, -1, 0, 0], [-1, 0, 0, 0]],
    [[0] * 4] * 4], np.float32)
chirality = np.array([1.0, 1.0, -1.0, -1.0], np.float32)


def color_apply(link_pair, spinor):
    link_re = link_pair[0][None]
    link_im = link_pair[1][None]
    part_re = spinor[0][:, None]
    part_im = spinor[1][:, None]
    real_part = jnp.sum(link_re * part_re - link_im * part_im, axis=2)
    imag_part = jnp.sum(link_re * part_im + link_im * part_re, axis=2)
    return jnp.stack([real_part, imag_part])


def apply_table(table_value, part_value):
    return jnp.tensordot(jnp.asarray(table_value), part_value, axes=([1], [0]), precision=lax.Precision.HIGHEST)


def spin_mix(spinor, direction):
    real_part = apply_table(gamma_real[direction], spinor[0]) - apply_table(gamma_imag[direction], spinor[1])
    imag_part = apply_table(gamma_real[direction], spinor[1]) + apply_table(gamma_imag[direction], spinor[0])
    return jnp.stack([real_part, imag_part])


def chirality_sign(spinor):
    return jnp.asarray(chirality).reshape((4,) + (1,) * (spinor.ndim - 2))


def twisted_diagonal(spinor):
    signs = chirality_sign(spinor)
    diagonal_value = 4.0 + quark_mass
    real_part = diagonal_value * spinor[0] - twist_mass * signs * spinor[1]
    imag_part = diagonal_value * spinor[1] + twist_mass * signs * spinor[0]
    return jnp.stack([real_part, imag_part])


def precondition(spinor):
    signs = chirality_sign(spinor)
    diagonal_value = 4.0 + quark_mass
    denominator = diagonal_value * diagonal_value + twist_mass * twist_mass
    real_part = (diagonal_value * spinor[0] + twist_mass * signs * spinor[1]) / denominator
    imag_part = (diagonal_value * spinor[1] - twist_mass * signs * spinor[0]) / denominator
    return jnp.stack([real_part, imag_part])


def wilson(spinor, ahead_list, behind_list, gauge_links):
    hopping = jnp.zeros_like(spinor)
    for direction in range(4):
        upward = color_apply(gauge_links[:, 2 * direction], ahead_list[direction])
        downward = color_apply(gauge_links[:, 2 * direction + 1], behind_list[direction])
        hopping = hopping + upward - spin_mix(upward, direction) + downward + spin_mix(downward, direction)
    return twisted_diagonal(spinor) - 0.5 * hopping


def fine_operator(spinor, gauge_links):
    ahead_list = [jnp.roll(spinor, -1, axis=3 + direction) for direction in range(4)]
    behind_list = [jnp.roll(spinor, 1, axis=3 + direction) for direction in range(4)]
    return wilson(spinor, ahead_list, behind_list, gauge_links)


def middle_layout(blocks):
    count = blocks.shape[2]
    split = blocks.reshape(blocks.shape[:6] + (count, blocks.shape[6] // count))
    return jnp.moveaxis(split, 6, 3)


def vector_layout(vectors):
    split = vectors.reshape(vectors.shape[:5] + (NVEC, vectors.shape[5] // NVEC))
    return jnp.moveaxis(split, 5, 2)


def bottom_layout(blocks):
    split = blocks.reshape(blocks.shape[:4] + (-1, NVEC2, NVEC2))
    return jnp.transpose(split, (0, 1, 5, 6, 2, 3, 4))


def block_apply(blocks, near_stack):
    def block_product(matrix, vector):
        return jnp.einsum('djk...,dk...->j...', matrix, vector, precision=lax.Precision.HIGHEST)
    real_part = block_product(blocks[0], near_stack[0]) - block_product(blocks[1], near_stack[1])
    imag_part = block_product(blocks[0], near_stack[1]) + block_product(blocks[1], near_stack[0])
    return jnp.stack([real_part, imag_part])


def restrict_middle(middle_vectors, coarse):
    def contract(left_side, right_side):
        return jnp.einsum('kjtzxa,jtzxa->ktzx', left_side, right_side, precision=lax.Precision.HIGHEST)
    real_part = contract(middle_vectors[0], coarse[0]) + contract(middle_vectors[1], coarse[1])
    imag_part = contract(middle_vectors[0], coarse[1]) - contract(middle_vectors[1], coarse[0])
    return jnp.stack([real_part, imag_part])


def prolong_middle(middle_vectors, coarse):
    def contract(left_side, right_side):
        return jnp.einsum('kjtzxa,ktzx->jtzxa', left_side, right_side, precision=lax.Precision.HIGHEST)
    real_part = contract(middle_vectors[0], coarse[0]) - contract(middle_vectors[1], coarse[1])
    imag_part = contract(middle_vectors[0], coarse[1]) + contract(middle_vectors[1], coarse[0])
    return jnp.stack([real_part, imag_part])


def inner_product(left_side, right_side):
    real_part = jnp.sum(left_side[0] * right_side[0] + left_side[1] * right_side[1])
    imag_part = jnp.sum(left_side[0] * right_side[1] - left_side[1] * right_side[0])
    return real_part, imag_part


def gram_partials(right_side, first_image, second_image):
    first_norm = inner_product(first_image, first_image)[0]
    second_norm = inner_product(second_image, second_image)[0]
    cross_re, cross_im = inner_product(first_image, second_image)
    first_re, first_im = inner_product(first_image, right_side)
    second_re, second_im = inner_product(second_image, right_side)
    return jnp.stack([first_norm, second_norm, cross_re, cross_im, first_re, first_im, second_re, second_im])


def complex_scale(coef_re, coef_im, vector):
    return jnp.stack([coef_re * vector[0] - coef_im * vector[1], coef_re * vector[1] + coef_im * vector[0]])


def least_squares(totals, right_side, first_image):
    first_norm = totals[0]
    second_norm = totals[1]
    cross_re = totals[2]
    cross_im = totals[3]
    first_re = totals[4]
    first_im = totals[5]
    second_re = totals[6]
    second_im = totals[7]
    determinant = first_norm * second_norm - cross_re * cross_re - cross_im * cross_im
    coef_one_re = (second_norm * first_re - (cross_re * second_re - cross_im * second_im)) / determinant
    coef_one_im = (second_norm * first_im - (cross_re * second_im + cross_im * second_re)) / determinant
    coef_two_re = (first_norm * second_re - (cross_re * first_re + cross_im * first_im)) / determinant
    coef_two_im = (first_norm * second_im - (cross_re * first_im - cross_im * first_re)) / determinant
    return complex_scale(coef_one_re, coef_one_im, right_side) + complex_scale(coef_two_re, coef_two_im, first_image)


def restrict_fine(residual_low, fine_vectors):
    split_vectors = fine_vectors.reshape((2, NVEC, 4, 3, N_TA, TL, N_GZ, ZL, N_XY, XL, YBLOCKS, BY))
    split_residual = residual_low.reshape((2, 4, 3, N_TA, TL, N_GZ, ZL, N_XY, XL, YBLOCKS, BY))
    collected = []
    for block in range(YBLOCKS):
        piece_vectors = split_vectors[..., block, :].astype(jnp.float32)
        piece_residual = split_residual[..., block, :].astype(jnp.float32)
        collected.append(jnp.einsum('pkscdefghib,qscdefghib->pqkdfh', piece_vectors, piece_residual,
                                    precision=lax.Precision.HIGHEST))
    terms = jnp.stack(collected, axis=-1)
    return jnp.stack([terms[0, 0] + terms[1, 1], terms[0, 1] - terms[1, 0]])


def prolong_fine(update_low, fine_vectors):
    split_vectors = fine_vectors.reshape((2, NVEC, 4, 3, N_TA, TL, N_GZ, ZL, N_XY, XL, YBLOCKS, BY))
    collected = []
    for block in range(YBLOCKS):
        piece_vectors = split_vectors[..., block, :].astype(jnp.float32)
        coefficients = update_low[..., block].astype(jnp.float32)
        terms = jnp.einsum('pkscdefghib,qkdfh->pqscdefghib', piece_vectors, coefficients,
                           precision=lax.Precision.HIGHEST)
        collected.append(jnp.stack([terms[0, 0] - terms[1, 1], terms[0, 1] + terms[1, 0]]))
    joined = jnp.stack(collected, axis=-2)
    return joined.reshape((2, 4, 3, NT, NZ, NX, YL))


def middle_operator(coarse, middle_blocks):
    near_list = [coarse]
    for axis_number in (2, 3, 4, 5):
        near_list.append(jnp.roll(coarse, -1, axis=axis_number))
        near_list.append(jnp.roll(coarse, 1, axis=axis_number))
    return middle_shift * coarse + block_apply(middle_blocks, jnp.stack(near_list, axis=1))


def bottom_operator(coarse, bottom_blocks):
    near_list = [coarse]
    for axis_number in (2, 3, 4):
        near_list.append(jnp.roll(coarse, -1, axis=axis_number))
        near_list.append(jnp.roll(coarse, 1, axis=axis_number))
    return bottom_shift * coarse + block_apply(bottom_blocks, jnp.stack(near_list, axis=1))


def reference(source_field, gauge_links, fine_vectors, middle_blocks, middle_vectors, bottom_blocks):
    middle_blocks = middle_layout(middle_blocks)
    middle_vectors = vector_layout(middle_vectors)
    bottom_blocks = bottom_layout(bottom_blocks)
    first_iterate = fine_damping * precondition(source_field)
    first_residual = source_field - fine_operator(first_iterate, gauge_links)
    second_iterate = first_iterate + fine_damping * precondition(first_residual)
    smoothed_residual = source_field - fine_operator(second_iterate, gauge_links)
    middle_right = restrict_fine(smoothed_residual.astype(jnp.bfloat16), fine_vectors)
    bottom_right = restrict_middle(middle_vectors, middle_right)
    first_image = bottom_operator(bottom_right, bottom_blocks)
    second_image = bottom_operator(first_image, bottom_blocks)
    totals = gram_partials(bottom_right, first_image, second_image)
    bottom_solution = least_squares(totals, bottom_right, first_image)
    middle_guess = prolong_middle(middle_vectors, bottom_solution)
    middle_update = middle_guess + middle_damping * (middle_right - middle_operator(middle_guess, middle_blocks))
    correction = prolong_fine(middle_update.astype(jnp.bfloat16), fine_vectors)
    return second_iterate + correction, smoothed_residual
```

```python
import functools

import jax
import jax.numpy as jnp
from jax import lax
from jax.experimental import pallas as pl
from jax.experimental.pallas import tpu as pltpu
from jax.sharding import PartitionSpec as P

BY = 4
NV = 24
NC = 3
NSC = 12

DIAGONAL = 4.0 + 0.1
TWIST = 0.1
DENOMINATOR = DIAGONAL * DIAGONAL + TWIST * TWIST
FINE_DAMPING = 0.8
MIDDLE_DAMPING = 0.4
MIDDLE_SHIFT = 2.0
BOTTOM_SHIFT = 2.0
MESH = pl.DeviceIdType.MESH
F32 = jnp.float32
BF16 = jnp.bfloat16
AXES = ("ta", "gz", "xy")


def plan(sizes):
    n_ta, n_gz, n_xy = sizes
    lines = []
    for offset in ((0, 0), (1, 0), (-1, 0), (0, 1), (0, -1)):
        reduced = (offset[0] % n_ta, offset[1] % n_gz)
        if reduced not in lines:
            lines.append(reduced)
    hops = []
    for axis in range(3):
        for step in (1, -1):
            offset = [0, 0, 0]
            offset[axis] = -step % sizes[axis]
            hops.append(tuple(offset))
    plane = [(a, b) for a in range(n_ta) for b in range(n_gz) if (a, b) != (0, 0)]
    spread = [(a, b, x) for a, b in lines for x in range(n_xy) if (a, b, x) != (0, 0, 0)]
    peers = []
    for offset in hops + [(a, b, 0) for a, b in plane] + spread:
        back = tuple(-o % n for o, n in zip(offset, sizes))
        for one in (offset, back):
            if one not in peers:
                peers.append(one)
    return lines, hops, plane, spread, peers


def dot(a, b, dims=((1,), (0,))):
    return lax.dot_general(
        a, b, (dims, ((), ())), precision=lax.Precision.HIGHEST, preferred_element_type=F32
    )


def split_dot(a, b, dims):
    high = a.astype(BF16)
    low = (a - high.astype(F32)).astype(BF16)
    rows = a.shape[0]
    both = lax.dot_general(
        jnp.concatenate([high, low], axis=0), b, (dims, ((), ())), preferred_element_type=F32
    )
    return both[:rows] + both[rows:]


def iota(shape, dim):
    return lax.broadcasted_iota(jnp.int32, shape, dim)


def hopping(load, gauge):
    row = iota((8, 128), 0)
    odd = (row & 1) == 1
    m = row >> 1
    near = m < 2
    eps = jnp.where(odd, 1.0, -1.0).astype(F32)

    def phase(values):
        re = jnp.zeros((8, 128), F32)
        im = jnp.zeros((8, 128), F32)
        for i, (a, b) in enumerate(values):
            re = jnp.where(m == i, a, re)
            im = jnp.where(m == i, b, im)
        return re * eps, im * eps

    up0 = phase(((1.0, 0.0), (0.0, 1.0), (0.0, 1.0), (-1.0, 0.0)))
    up1 = phase(((1.0, 0.0), (0.0, -1.0), (0.0, 1.0), (1.0, 0.0)))
    low2 = phase(((1.0, 0.0), (0.0, -1.0), (0.0, -1.0), (1.0, 0.0)))
    low3 = phase(((1.0, 0.0), (0.0, 1.0), (0.0, -1.0), (-1.0, 0.0)))

    def times(c, re, im):
        return c[0] * re - c[1] * im, c[0] * im + c[1] * re

    half = {}
    for color in range(NC):
        v = [load(spin, color) for spin in range(4)]
        for spin, c in ((0, up0), (1, up1)):
            first, other = (v[2], v[3]) if spin == 0 else (v[3], v[2])
            re = jnp.where(near, first[0], other[0])
            im = jnp.where(near, first[1], other[1])
            re, im = times(c, re, im)
            half[spin, color] = (v[spin][0] + re, v[spin][1] + im)
    out = {}
    for c in range(NC):
        acc = {0: None, 1: None}
        for k in range(NC):
            ure = gauge[pl.ds(c * 3 + k, 8, stride=9), :]
            uim = gauge[pl.ds(72 + c * 3 + k, 8, stride=9), :]
            for spin in range(2):
                hre, him = half[spin, k]
                re = ure * hre - uim * him
                im = ure * him + uim * hre
                acc[spin] = (re, im) if acc[spin] is None else (acc[spin][0] + re, acc[spin][1] + im)
        w0, w1 = acc[0], acc[1]
        out[0, c] = w0
        out[1, c] = w1
        for spin, coef in ((2, low2), (3, low3)):
            first, other = (w0, w1) if spin == 2 else (w1, w0)
            re = jnp.where(near, first[0], other[0])
            im = jnp.where(near, first[1], other[1])
            out[spin, c] = times(coef, re, im)
    rows = [
        jnp.sum(out[spin, c][part], axis=0, keepdims=True)
        for part in range(2)
        for spin in range(4)
        for c in range(NC)
    ]
    return jnp.concatenate(rows, axis=0)


def signs_of():
    row = iota((24, 128), 0)
    inner = jnp.where(row >= NSC, row - NSC, row)
    return jnp.where(inner < 6, 1.0, -1.0).astype(F32), row < NSC


def swap(v):
    return jnp.concatenate([v[NSC:], v[:NSC]], axis=0)


def twisted(v):
    g5, real = signs_of()
    return DIAGONAL * v + TWIST * jnp.where(real, -g5, g5) * swap(v)


def precondition(v):
    g5, real = signs_of()
    return (DIAGONAL * v + TWIST * jnp.where(real, g5, -g5) * swap(v)) * (1.0 / DENOMINATOR)


def kernel(
    sizes, source, gauge_hbm, fine, mb_hbm, mv_hbm, bb_hbm,
    solution_ref, residual_ref,
    gauge, mb, mv, bb, fine32, near1, near2, second, expand, reduce,
    rsend, rbuf, fsend, fbuf, psend, pbuf, tsend, tbuf,
    local_sem, send_sem, recv_sem,
):
    n_ta, n_gz, n_xy = sizes
    lines, hops, plane, spread, peers = plan(sizes)
    me = tuple(lax.axis_index(a) for a in AXES)
    chunks = n_xy * NV * NV // 128
    width = rsend.shape[1]

    def device(offset):
        return tuple(lax.rem(m + o, n) for m, o, n in zip(me, offset, sizes))

    loads = [
        pltpu.make_async_copy(gauge_hbm, gauge, local_sem.at[0]),
        pltpu.make_async_copy(mb_hbm, mb, local_sem.at[1]),
        pltpu.make_async_copy(mv_hbm, mv, local_sem.at[2]),
        pltpu.make_async_copy(bb_hbm, bb.at[pl.ds(0, 14 * chunks)], local_sem.at[3]),
    ]
    barrier = pltpu.get_barrier_semaphore()
    for offset in peers:
        pl.semaphore_signal(barrier, inc=1, device_id=device(offset), device_id_type=MESH)
    for load in loads:
        load.start()

    bb[pl.ds(14 * chunks, bb.shape[0] - 14 * chunks), :] = jnp.zeros(
        (bb.shape[0] - 14 * chunks, 128), F32
    )
    count = [0]

    def send(src, dst, offset):
        copy = pltpu.make_async_remote_copy(
            src_ref=src, dst_ref=dst, send_sem=send_sem.at[count[0]],
            recv_sem=recv_sem.at[count[0]], device_id=device(offset), device_id_type=MESH,
        )
        count[0] += 1
        copy.start()
        return copy

    pl.semaphore_wait(barrier, len(peers))
    pending = []

    def halo(src, buf):
        return [send(src, buf.at[pl.ds(24 * i, 24)], offset) for i, offset in enumerate(hops)]

    def fill_y(v, buf):
        buf[pl.ds(24 * 6, 24), :] = pltpu.roll(v, 127, 1)
        buf[pl.ds(24 * 7, 24), :] = pltpu.roll(v, 1, 1)

    copies1 = halo(source, near1)
    pending += copies1
    src = source[...]
    fill_y(src, near1)
    first = FINE_DAMPING * precondition(src)

    cols = n_xy * NV * NV
    n = iota((1, cols), 1).astype(F32)
    xs = jnp.floor((n + 0.5) * (1.0 / (NV * NV)))
    js = jnp.floor((n - xs * (NV * NV) + 0.5) * (1.0 / NV))
    ks = n - xs * (NV * NV) - js * NV
    lane = iota((width, cols), 0).astype(F32)
    expand[...] = jnp.where(lane == xs * NV + ks, 1.0, 0.0).astype(BF16)
    reduce[...] = jnp.where(lane == xs * NV + js, 1.0, 0.0).astype(BF16)
    fine32[...] = fine[...].astype(F32)

    def loader(buf, scaled):
        def load(spin, color):
            i = spin * NC + color
            re = buf[pl.ds(i, 8, stride=24), :]
            im = buf[pl.ds(NSC + i, 8, stride=24), :]
            if not scaled:
                return re, im
            a = FINE_DAMPING * DIAGONAL / DENOMINATOR
            b = FINE_DAMPING * TWIST / DENOMINATOR * (1.0 if spin < 2 else -1.0)
            return a * re + b * im, a * im - b * re
        return load

    loads[0].wait()
    for copy in copies1:
        copy.wait_recv()
    hop = hopping(loader(near1, True), gauge)
    second_value = first + FINE_DAMPING * precondition(src - (twisted(first) - 0.5 * hop))
    second[...] = second_value
    copies2 = halo(second, near2)
    pending += copies2
    fill_y(second_value, near2)
    loads[2].wait()
    loads[3].wait()
    loads[1].wait()
    for copy in copies2:
        copy.wait_recv()
    hop = hopping(loader(near2, False), gauge)
    smoothed = src - (twisted(second_value) - 0.5 * hop)
    residual_ref[...] = smoothed
    low = smoothed.astype(BF16).astype(F32)

    mre = jnp.zeros((NV, 128), F32)
    mim = jnp.zeros((NV, 128), F32)
    for i in range(NSC):
        fre = fine32[pl.ds(i, NV, stride=NSC), :]
        fim = fine32[pl.ds(NV * NSC + i, NV, stride=NSC), :]
        rre, rim = low[i : i + 1], low[NSC + i : NSC + i + 1]
        mre = mre + fre * rre + fim * rim
        mim = mim + fre * rim - fim * rre
    sums = jnp.concatenate([mre, mim], axis=0)
    li = iota((128, 128), 0)
    lj = iota((128, 128), 1)
    group = jnp.where((li >> 2) == (lj & 31), 1.0, 0.0).astype(F32)
    rep = dot(sums, group)
    own_group = ((iota((48, 128), 0) & 3) == (iota((48, 128), 1) >> 5))
    masked = jnp.where(own_group, rep, 0.0)
    gather = jnp.where(iota((16, 48), 0) == (iota((16, 48), 1) >> 2), 1.0, 0.0).astype(F32)
    mr = dot(gather, masked)

    are = jnp.zeros((NV, 128), F32)
    aim = jnp.zeros((NV, 128), F32)
    for c in range(6):
        vre = mv[pl.ds(c, NV, stride=6), :]
        vim = mv[pl.ds(NV * 6 + c, NV, stride=6), :]
        rre, rim = mr[c : c + 1], mr[6 + c : 7 + c]
        are = are + vre * rre + vim * rim
        aim = aim + vre * rim - vim * rre
    rcol_re = jnp.sum(are, axis=1, keepdims=True)
    rcol_im = jnp.sum(aim, axis=1, keepdims=True)
    place = iota((NV, width), 1) == me[2] * NV + iota((NV, width), 0)
    own_re = jnp.sum(jnp.where(place, rcol_re, 0.0), axis=0, keepdims=True)
    own_im = jnp.sum(jnp.where(place, rcol_im, 0.0), axis=0, keepdims=True)
    tile_row = iota((8, width), 0)

    def pair_tile(re, im):
        return jnp.where(tile_row == 0, re, jnp.where(tile_row == 1, im, 0.0))

    own_tile = pair_tile(own_re, own_im)
    rsend[...] = own_tile
    copies3 = []
    for a, b, x in spread:
        slot = lines.index((-a % n_ta, -b % n_gz))
        copies3.append(send(rsend, rbuf.at[slot * n_xy + x], (a, b, x)))
    pending += copies3

    def prolong(re, im):
        re = jnp.broadcast_to(re, (NV, 128))
        im = jnp.broadcast_to(im, (NV, 128))
        rows_re, rows_im = [], []
        for c in range(6):
            vre = mv[pl.ds(c, NV, stride=6), :]
            vim = mv[pl.ds(NV * 6 + c, NV, stride=6), :]
            rows_re.append(jnp.sum(vre * re - vim * im, axis=0, keepdims=True))
            rows_im.append(jnp.sum(vre * im + vim * re, axis=0, keepdims=True))
        zero = jnp.zeros((2, 128), F32)
        return jnp.concatenate(rows_re + [zero] + rows_im + [zero], axis=0)

    psend[pl.ds(0, 16), :] = prolong(rcol_re, rcol_im)

    for copy in copies3:
        copy.wait_recv()

    def line_slot(offset):
        return lines.index((offset[0] % n_ta, offset[1] % n_gz))

    near_offsets = ((1, 0), (-1, 0), (0, 1), (0, -1))
    length = n_xy * NV

    def turn(v, shift):
        lanes = iota(v.shape, 1)
        if shift > 0:
            inside, wrapped = lanes < length - shift, length - shift
            one, two = pltpu.roll(v, width - shift, 1), pltpu.roll(v, wrapped, 1)
        else:
            inside = lanes >= -shift
            one, two = pltpu.roll(v, -shift, 1), pltpu.roll(v, width - (length + shift), 1)
        return jnp.where(lanes < length, jnp.where(inside, one, two), 0.0)

    def bottom(own, others):
        near = [own] + others + [turn(own, NV), turn(own, -NV)]
        zero = jnp.zeros((1, width), F32)
        stack = jnp.concatenate(
            [v[0:1] for v in near] + [zero] + [v[1:2] for v in near] + [zero], axis=0
        )
        wide = split_dot(stack, expand[...], ((1,), (0,)))
        parts = []
        for c in range(chunks):
            bre = bb[pl.ds(c, 8, stride=chunks), :]
            bim = bb[pl.ds(7 * chunks + c, 8, stride=chunks), :]
            vre = wide[0:8, c * 128 : (c + 1) * 128]
            vim = wide[8:16, c * 128 : (c + 1) * 128]
            parts.append(jnp.concatenate([bre * vre - bim * vim, bre * vim + bim * vre], axis=0))
        prod = jnp.concatenate(parts, axis=1)
        short = split_dot(prod, reduce[...], ((1,), (1,)))
        re = jnp.sum(short[0:8], axis=0, keepdims=True)
        im = jnp.sum(short[8:16], axis=0, keepdims=True)
        return pair_tile(re, im) + BOTTOM_SHIFT * own

    def gathered(slot):
        total = own_tile if slot == 0 else rbuf[slot * n_xy]
        for x in range(1, n_xy):
            total = total + rbuf[slot * n_xy + x]
        return total

    slots = [gathered(s) for s in range(len(lines))]
    r = slots[0]
    f = bottom(r, [slots[line_slot(o)] for o in near_offsets])
    fsend[...] = f
    copies4 = []
    for i, (a, b) in enumerate(lines):
        if i:
            copies4.append(send(fsend, fbuf.at[lines.index((-a % n_ta, -b % n_gz))], (a, b, 0)))
    pending += copies4
    fcol_re = jnp.sum(jnp.where(place, f[0:1], 0.0), axis=1, keepdims=True)
    fcol_im = jnp.sum(jnp.where(place, f[1:2], 0.0), axis=1, keepdims=True)
    psend[pl.ds(16, 16), :] = prolong(fcol_re, fcol_im)
    copies5 = [send(psend, pbuf.at[pl.ds(32 * i, 32)], offset) for i, offset in enumerate(hops)]
    pending += copies5
    for copy in copies4:
        copy.wait_recv()
    s = bottom(f, [fbuf[line_slot(o)] for o in near_offsets])

    rr, ri, fr, fi, sr, si = r[0:1], r[1:2], f[0:1], f[1:2], s[0:1], s[1:2]
    tsend[...] = jnp.concatenate(
        [
            fr * fr + fi * fi,
            sr * sr + si * si,
            fr * sr + fi * si,
            fr * si - fi * sr,
            fr * rr + fi * ri,
            fr * ri - fi * rr,
            sr * rr + si * ri,
            sr * ri - si * rr,
        ],
        axis=0,
    )
    copies6 = []
    for i, (a, b) in enumerate(plane):
        copies6.append(send(tsend, tbuf.at[i], (a, b, 0)))
    pending += copies6

    own_p = psend[...]
    lane32 = iota((32, 128), 1) & 31
    y_up = jnp.where(lane32 == 31, pltpu.roll(own_p, 31, 1), pltpu.roll(own_p, 127, 1))
    y_down = jnp.where(lane32 == 0, pltpu.roll(own_p, 97, 1), pltpu.roll(own_p, 1, 1))
    acc = [jnp.zeros((NV, 128), F32) for _ in range(4)]

    def add_direction(acc, d, v):
        acc = list(acc)
        for c in range(6):
            bre = mb[pl.ds(d * NV * 6 + c, NV, stride=6), :]
            bim = mb[pl.ds((9 + d) * NV * 6 + c, NV, stride=6), :]
            for image in range(2):
                vre = v[16 * image + c : 16 * image + c + 1]
                vim = v[16 * image + 8 + c : 16 * image + 9 + c]
                acc[2 * image] = acc[2 * image] + bre * vre - bim * vim
                acc[2 * image + 1] = acc[2 * image + 1] + bre * vim + bim * vre
        return acc

    acc = add_direction(acc, 0, own_p)
    acc = add_direction(acc, 7, y_up)
    acc = add_direction(acc, 8, y_down)
    for copy in copies5:
        copy.wait_recv()
    for i in range(6):
        acc = add_direction(acc, 1 + i, pbuf[pl.ds(32 * i, 32), :])
    lift = jnp.where(
        (iota((96, 32), 1) >> 3) == (iota((96, 32), 0).astype(F32) * (1.0 / NV) + 1e-3).astype(jnp.int32),
        1.0, 0.0,
    ).astype(F32)
    rows96 = iota((96, 32), 0)
    inner = rows96 - NV * (rows96.astype(F32) * (1.0 / NV) + 1e-3).astype(jnp.int32)
    lift = jnp.where((inner >> 2) == (iota((96, 32), 1) & 7), lift, 0.0)
    spread_p = dot(lift, own_p)
    keep = (iota((96, 128), 0) & 3) == (iota((96, 128), 1) >> 5)
    z = jnp.where(keep, spread_p, 0.0) * (1.0 - MIDDLE_DAMPING * MIDDLE_SHIFT)
    z = z - MIDDLE_DAMPING * jnp.concatenate(acc, axis=0)
    to_sites = jnp.where((li & 31) == (lj >> 2), 1.0, 0.0).astype(F32)
    u = dot(z, to_sites)
    same = jnp.where((li >> 2) == (lj >> 2), MIDDLE_DAMPING, 0.0).astype(F32)
    base = dot(sums, same)

    for copy in copies6:
        copy.wait_recv()
    total = tsend[...]
    for i in range(len(plane)):
        total = total + tbuf[i]
    total = jnp.sum(total, axis=1, keepdims=True)
    t = [total[i : i + 1] for i in range(8)]
    ff, ss, cre, cim, f_re, f_im, s_re, s_im = t
    det = ff * ss - cre * cre - cim * cim
    c1r = (ss * f_re - (cre * s_re - cim * s_im)) / det
    c1i = (ss * f_im - (cre * s_im + cim * s_re)) / det
    c2r = (ff * s_re - (cre * f_re + cim * f_im)) / det
    c2i = (ff * s_im - (cre * f_im - cim * f_re)) / det
    ur_re, ur_im, uf_re, uf_im = (u[NV * q : NV * (q + 1)] for q in range(4))
    up_re = base[:NV] + c1r * ur_re - c1i * ur_im + c2r * uf_re - c2i * uf_im
    up_im = base[NV:] + c1r * ur_im + c1i * ur_re + c2r * uf_im + c2i * uf_re
    up_re = up_re.astype(BF16).astype(F32)
    up_im = up_im.astype(BF16).astype(F32)
    out_re = second_value[:NSC]
    out_im = second_value[NSC:]
    for k in range(NV):
        fre = fine32[pl.ds(k * NSC, NSC), :]
        fim = fine32[pl.ds((NV + k) * NSC, NSC), :]
        a, b = up_re[k : k + 1], up_im[k : k + 1]
        out_re = out_re + fre * a - fim * b
        out_im = out_im + fre * b + fim * a
    solution_ref[...] = jnp.concatenate([out_re, out_im], axis=0)
    for copy in pending:
        copy.wait_send()


def shards(sizes, source_field, gauge_links, fine_vectors, middle_blocks, middle_vectors, bottom_blocks):
    lines, hops, plane, spread, peers = plan(sizes)
    n_xy = sizes[2]
    chunks = n_xy * NV * NV // 128
    width = -(-n_xy * NV // 128) * 128
    copies = 3 * len(hops) + len(spread) + len(lines) - 1 + len(plane)
    vmem = pl.BlockSpec(memory_space=pltpu.VMEM)
    hbm = pl.BlockSpec(memory_space=pl.ANY)
    out = jax.ShapeDtypeStruct((24, 128), F32)
    results = pl.pallas_call(
        functools.partial(kernel, sizes),
        out_shape=(out, out),
        in_specs=[vmem, hbm, vmem, hbm, hbm, hbm],
        out_specs=(vmem, vmem),
        scratch_shapes=[
            pltpu.VMEM((144, 128), F32),
            pltpu.VMEM((2 * 9 * NV * 6, 128), F32),
            pltpu.VMEM((2 * NV * 6, 128), F32),
            pltpu.VMEM(((15 * chunks + 7) // 8 * 8, 128), F32),
            pltpu.VMEM((2 * NV * NSC, 128), F32),
            pltpu.VMEM((192, 128), F32),
            pltpu.VMEM((192, 128), F32),
            pltpu.VMEM((24, 128), F32),
            pltpu.VMEM((width, n_xy * NV * NV), BF16),
            pltpu.VMEM((width, n_xy * NV * NV), BF16),
            pltpu.VMEM((8, width), F32),
            pltpu.VMEM((len(lines) * n_xy, 8, width), F32),
            pltpu.VMEM((8, width), F32),
            pltpu.VMEM((len(lines), 8, width), F32),
            pltpu.VMEM((32, 128), F32),
            pltpu.VMEM((6 * 32, 128), F32),
            pltpu.VMEM((8, width), F32),
            pltpu.VMEM((len(plane), 8, width), F32),
            pltpu.SemaphoreType.DMA((4,)),
            pltpu.SemaphoreType.DMA((copies,)),
            pltpu.SemaphoreType.DMA((copies,)),
        ],
        compiler_params=pltpu.CompilerParams(
            collective_id=0, has_side_effects=True, vmem_limit_bytes=60 * 1024 * 1024
        ),
    )(
        source_field.reshape(24, 128),
        gauge_links.reshape(144, 128),
        fine_vectors.reshape(2 * NV * NSC, 128),
        middle_blocks.reshape(-1, 128),
        middle_vectors.reshape(-1, 128),
        bottom_blocks.reshape(-1, 128),
    )
    return tuple(x.reshape(source_field.shape) for x in results)


def solution(mesh):
    sizes = tuple(mesh.shape[a] for a in AXES)
    return jax.shard_map(
        functools.partial(shards, sizes),
        mesh=mesh,
        in_specs=(
            P(None, None, None, "ta", "gz", "xy", None),
            P(None, None, None, None, "ta", "gz", "xy", None),
            P(None, None, None, None, "ta", "gz", "xy", None),
            P(None, None, None, "ta", "gz", "xy", None),
            P(None, None, "ta", "gz", "xy", None),
            P(None, None, "ta", "gz", None),
        ),
        out_specs=(
            P(None, None, None, "ta", "gz", "xy", None),
            P(None, None, None, "ta", "gz", "xy", None),
        ),
        check_vma=False,
    )
```

```python
import functools

import jax
import jax.numpy as jnp
from jax import lax
from jax.experimental import pallas as pl
from jax.experimental.pallas import tpu as pltpu
from jax.sharding import PartitionSpec as P

BY = 4
NV = 24
NC = 3
NSC = 12

DIAGONAL = 4.0 + 0.1
TWIST = 0.1
DENOMINATOR = DIAGONAL * DIAGONAL + TWIST * TWIST
FINE_DAMPING = 0.8
MIDDLE_DAMPING = 0.4
MIDDLE_SHIFT = 2.0
BOTTOM_SHIFT = 2.0
MESH = pl.DeviceIdType.MESH
F32 = jnp.float32
BF16 = jnp.bfloat16
AXES = ("ta", "gz", "xy")


def plan(sizes):
    n_ta, n_gz, n_xy = sizes
    lines = []
    for offset in ((0, 0), (1, 0), (-1, 0), (0, 1), (0, -1)):
        reduced = (offset[0] % n_ta, offset[1] % n_gz)
        if reduced not in lines:
            lines.append(reduced)
    hops = []
    for axis in range(3):
        for step in (1, -1):
            offset = [0, 0, 0]
            offset[axis] = -step % sizes[axis]
            hops.append(tuple(offset))
    plane = [(a, b) for a in range(n_ta) for b in range(n_gz) if (a, b) != (0, 0)]
    spread = [(a, b, x) for a, b in lines for x in range(n_xy) if (a, b, x) != (0, 0, 0)]
    def distance(offset):
        return sum(min(o, n - o) for o, n in zip(offset, sizes))

    far = [o for o in [(a, b, 0) for a, b in plane] + spread if distance(o) > 3]
    peers = []
    for offset in hops + far:
        back = tuple(-o % n for o, n in zip(offset, sizes))
        for one in (offset, back):
            if one not in peers:
                peers.append(one)
    return lines, hops, plane, spread, peers


def dot(a, b, dims=((1,), (0,))):
    return lax.dot_general(
        a, b, (dims, ((), ())), precision=lax.Precision.HIGHEST, preferred_element_type=F32
    )


def split_dot(a, b, dims):
    high = a.astype(BF16)
    low = (a - high.astype(F32)).astype(BF16)
    rows = a.shape[0]
    both = lax.dot_general(
        jnp.concatenate([high, low], axis=0), b, (dims, ((), ())), preferred_element_type=F32
    )
    return both[:rows] + both[rows:]


def iota(shape, dim):
    return lax.broadcasted_iota(jnp.int32, shape, dim)


def hopping(load, gauge):
    row = iota((8, 128), 0)
    odd = (row & 1) == 1
    m = row >> 1
    near = m < 2
    eps = jnp.where(odd, 1.0, -1.0).astype(F32)

    def phase(values):
        re = jnp.zeros((8, 128), F32)
        im = jnp.zeros((8, 128), F32)
        for i, (a, b) in enumerate(values):
            re = jnp.where(m == i, a, re)
            im = jnp.where(m == i, b, im)
        return re * eps, im * eps

    up0 = phase(((1.0, 0.0), (0.0, 1.0), (0.0, 1.0), (-1.0, 0.0)))
    up1 = phase(((1.0, 0.0), (0.0, -1.0), (0.0, 1.0), (1.0, 0.0)))
    low2 = phase(((1.0, 0.0), (0.0, -1.0), (0.0, -1.0), (1.0, 0.0)))
    low3 = phase(((1.0, 0.0), (0.0, 1.0), (0.0, -1.0), (-1.0, 0.0)))

    def times(c, re, im):
        return c[0] * re - c[1] * im, c[0] * im + c[1] * re

    half = {}
    for color in range(NC):
        v = [load(spin, color) for spin in range(4)]
        for spin, c in ((0, up0), (1, up1)):
            first, other = (v[2], v[3]) if spin == 0 else (v[3], v[2])
            re = jnp.where(near, first[0], other[0])
            im = jnp.where(near, first[1], other[1])
            re, im = times(c, re, im)
            half[spin, color] = (v[spin][0] + re, v[spin][1] + im)
    out = {}
    for c in range(NC):
        acc = {0: None, 1: None}
        for k in range(NC):
            ure = gauge[pl.ds(c * 3 + k, 8, stride=9), :]
            uim = gauge[pl.ds(72 + c * 3 + k, 8, stride=9), :]
            for spin in range(2):
                hre, him = half[spin, k]
                re = ure * hre - uim * him
                im = ure * him + uim * hre
                acc[spin] = (re, im) if acc[spin] is None else (acc[spin][0] + re, acc[spin][1] + im)
        w0, w1 = acc[0], acc[1]
        out[0, c] = w0
        out[1, c] = w1
        for spin, coef in ((2, low2), (3, low3)):
            first, other = (w0, w1) if spin == 2 else (w1, w0)
            re = jnp.where(near, first[0], other[0])
            im = jnp.where(near, first[1], other[1])
            out[spin, c] = times(coef, re, im)
    rows = [
        jnp.sum(out[spin, c][part], axis=0, keepdims=True)
        for part in range(2)
        for spin in range(4)
        for c in range(NC)
    ]
    return jnp.concatenate(rows, axis=0)


def signs_of():
    row = iota((24, 128), 0)
    inner = jnp.where(row >= NSC, row - NSC, row)
    return jnp.where(inner < 6, 1.0, -1.0).astype(F32), row < NSC


def swap(v):
    return jnp.concatenate([v[NSC:], v[:NSC]], axis=0)


def twisted(v):
    g5, real = signs_of()
    return DIAGONAL * v + TWIST * jnp.where(real, -g5, g5) * swap(v)


def precondition(v):
    g5, real = signs_of()
    return (DIAGONAL * v + TWIST * jnp.where(real, g5, -g5) * swap(v)) * (1.0 / DENOMINATOR)


def kernel(
    sizes, source, gauge_hbm, fine_hbm, mb_hbm, mv_hbm, bb_hbm,
    result_ref,
    gauge, fine, mb, mv, bb, fine32, near1, near2, second, expand, reduce,
    rsend, rbuf, fsend, fbuf, psend, pbuf, tsend, tbuf,
    local_sem, send_sem, recv_sem,
):
    n_ta, n_gz, n_xy = sizes
    lines, hops, plane, spread, peers = plan(sizes)
    me = tuple(lax.axis_index(a) for a in AXES)
    chunks = n_xy * NV * NV // 128
    width = rsend.shape[1]

    def device(offset):
        return tuple(lax.rem(m + o, n) for m, o, n in zip(me, offset, sizes))

    loads = [
        pltpu.make_async_copy(gauge_hbm, gauge, local_sem.at[0]),
        pltpu.make_async_copy(mb_hbm, mb, local_sem.at[1]),
        pltpu.make_async_copy(mv_hbm, mv, local_sem.at[2]),
        pltpu.make_async_copy(bb_hbm.at[:, 0, :], bb.at[pl.ds(0, 14 * chunks)], local_sem.at[3]),
    ]
    fine_copy = pltpu.make_async_copy(fine_hbm, fine, local_sem.at[4])
    loads.append(fine_copy)
    barrier = pltpu.get_barrier_semaphore()
    for offset in peers:
        pl.semaphore_signal(barrier, inc=1, device_id=device(offset), device_id_type=MESH)
    for load in loads:
        load.start()

    bb[pl.ds(14 * chunks, bb.shape[0] - 14 * chunks), :] = jnp.zeros(
        (bb.shape[0] - 14 * chunks, 128), F32
    )
    count = [0]

    def send(src, dst, offset):
        copy = pltpu.make_async_remote_copy(
            src_ref=src, dst_ref=dst, send_sem=send_sem.at[count[0]],
            recv_sem=recv_sem.at[count[0]], device_id=device(offset), device_id_type=MESH,
        )
        count[0] += 1
        copy.start()
        return copy

    pl.semaphore_wait(barrier, len(peers))
    pending = []

    def halo(src, buf):
        return [send(src, buf.at[pl.ds(24 * i, 24)], offset) for i, offset in enumerate(hops)]

    def fill_y(v, buf):
        buf[pl.ds(24 * 6, 24), :] = pltpu.roll(v, 127, 1)
        buf[pl.ds(24 * 7, 24), :] = pltpu.roll(v, 1, 1)

    copies1 = halo(source, near1)
    pending += copies1
    src = source[...]
    fill_y(src, near1)
    first = FINE_DAMPING * precondition(src)

    cols = n_xy * NV * NV
    n = iota((1, cols), 1).astype(F32)
    xs = jnp.floor((n + 0.5) * (1.0 / (NV * NV)))
    js = jnp.floor((n - xs * (NV * NV) + 0.5) * (1.0 / NV))
    ks = n - xs * (NV * NV) - js * NV
    lane = iota((width, cols), 0).astype(F32)
    expand[...] = jnp.where(lane == xs * NV + ks, 1.0, 0.0).astype(BF16)
    reduce[...] = jnp.where(lane == xs * NV + js, 1.0, 0.0).astype(BF16)
    fine_copy.wait()
    fine32[...] = fine[...].astype(F32).reshape(2 * NV * NSC, 128)

    def loader(buf, scaled):
        def load(spin, color):
            i = spin * NC + color
            re = buf[pl.ds(i, 8, stride=24), :]
            im = buf[pl.ds(NSC + i, 8, stride=24), :]
            if not scaled:
                return re, im
            a = FINE_DAMPING * DIAGONAL / DENOMINATOR
            b = FINE_DAMPING * TWIST / DENOMINATOR * (1.0 if spin < 2 else -1.0)
            return a * re + b * im, a * im - b * re
        return load

    loads[0].wait()
    for copy in copies1:
        copy.wait_recv()
    hop = hopping(loader(near1, True), gauge)
    second_value = first + FINE_DAMPING * precondition(src - (twisted(first) - 0.5 * hop))
    second[...] = second_value
    copies2 = halo(second, near2)
    pending += copies2
    fill_y(second_value, near2)
    loads[2].wait()
    loads[3].wait()
    loads[1].wait()
    for copy in copies2:
        copy.wait_recv()
    hop = hopping(loader(near2, False), gauge)
    smoothed = src - (twisted(second_value) - 0.5 * hop)
    result_ref[pl.ds(24, 24), :] = smoothed
    low = smoothed.astype(BF16).astype(F32)

    mre = jnp.zeros((NV, 128), F32)
    mim = jnp.zeros((NV, 128), F32)
    for i in range(NSC):
        fre = fine32[pl.ds(i, NV, stride=NSC), :]
        fim = fine32[pl.ds(NV * NSC + i, NV, stride=NSC), :]
        at = i % 4 * NC + i // 4
        rre, rim = low[at : at + 1], low[NSC + at : NSC + at + 1]
        mre = mre + fre * rre + fim * rim
        mim = mim + fre * rim - fim * rre
    sums = jnp.concatenate([mre, mim], axis=0)
    li = iota((128, 128), 0)
    lj = iota((128, 128), 1)
    group = jnp.where((li >> 2) == (lj & 31), 1.0, 0.0).astype(F32)
    rep = dot(sums, group)
    own_group = ((iota((48, 128), 0) & 3) == (iota((48, 128), 1) >> 5))
    masked = jnp.where(own_group, rep, 0.0)
    gather = jnp.where(iota((16, 48), 0) == (iota((16, 48), 1) >> 2), 1.0, 0.0).astype(F32)
    mr = dot(gather, masked)

    are = jnp.zeros((NV, 128), F32)
    aim = jnp.zeros((NV, 128), F32)
    for c in range(6):
        vre = mv[pl.ds(c, NV, stride=6), :]
        vim = mv[pl.ds(NV * 6 + c, NV, stride=6), :]
        rre, rim = mr[c : c + 1], mr[6 + c : 7 + c]
        are = are + vre * rre + vim * rim
        aim = aim + vre * rim - vim * rre
    rcol_re = jnp.sum(are, axis=1, keepdims=True)
    rcol_im = jnp.sum(aim, axis=1, keepdims=True)
    place = iota((NV, width), 1) == me[2] * NV + iota((NV, width), 0)
    own_re = jnp.sum(jnp.where(place, rcol_re, 0.0), axis=0, keepdims=True)
    own_im = jnp.sum(jnp.where(place, rcol_im, 0.0), axis=0, keepdims=True)
    tile_row = iota((8, width), 0)

    def pair_tile(re, im):
        return jnp.where(tile_row == 0, re, jnp.where(tile_row == 1, im, 0.0))

    own_tile = pair_tile(own_re, own_im)
    rsend[...] = own_tile
    copies3 = []
    for a, b, x in spread:
        slot = lines.index((-a % n_ta, -b % n_gz))
        copies3.append(send(rsend, rbuf.at[slot * n_xy + x], (a, b, x)))
    pending += copies3

    def prolong(re, im):
        re = jnp.broadcast_to(re, (NV, 128))
        im = jnp.broadcast_to(im, (NV, 128))
        rows_re, rows_im = [], []
        for c in range(6):
            vre = mv[pl.ds(c, NV, stride=6), :]
            vim = mv[pl.ds(NV * 6 + c, NV, stride=6), :]
            rows_re.append(jnp.sum(vre * re - vim * im, axis=0, keepdims=True))
            rows_im.append(jnp.sum(vre * im + vim * re, axis=0, keepdims=True))
        zero = jnp.zeros((2, 128), F32)
        return jnp.concatenate(rows_re + [zero] + rows_im + [zero], axis=0)

    psend[pl.ds(0, 16), :] = prolong(rcol_re, rcol_im)

    for copy in copies3:
        copy.wait_recv()

    def line_slot(offset):
        return lines.index((offset[0] % n_ta, offset[1] % n_gz))

    near_offsets = ((1, 0), (-1, 0), (0, 1), (0, -1))
    length = n_xy * NV

    def turn(v, shift):
        lanes = iota(v.shape, 1)
        if shift > 0:
            inside, wrapped = lanes < length - shift, length - shift
            one, two = pltpu.roll(v, width - shift, 1), pltpu.roll(v, wrapped, 1)
        else:
            inside = lanes >= -shift
            one, two = pltpu.roll(v, -shift, 1), pltpu.roll(v, width - (length + shift), 1)
        return jnp.where(lanes < length, jnp.where(inside, one, two), 0.0)

    def bottom(own, others):
        near = [own] + others + [turn(own, NV), turn(own, -NV)]
        zero = jnp.zeros((1, width), F32)
        stack = jnp.concatenate(
            [v[0:1] for v in near] + [zero] + [v[1:2] for v in near] + [zero], axis=0
        )
        wide = split_dot(stack, expand[...], ((1,), (0,)))
        parts = []
        for c in range(chunks):
            bre = bb[pl.ds(c, 8, stride=chunks), :]
            bim = bb[pl.ds(7 * chunks + c, 8, stride=chunks), :]
            vre = wide[0:8, c * 128 : (c + 1) * 128]
            vim = wide[8:16, c * 128 : (c + 1) * 128]
            parts.append(jnp.concatenate([bre * vre - bim * vim, bre * vim + bim * vre], axis=0))
        prod = jnp.concatenate(parts, axis=1)
        short = split_dot(prod, reduce[...], ((1,), (1,)))
        re = jnp.sum(short[0:8], axis=0, keepdims=True)
        im = jnp.sum(short[8:16], axis=0, keepdims=True)
        return pair_tile(re, im) + BOTTOM_SHIFT * own

    def gathered(slot):
        total = own_tile if slot == 0 else rbuf[slot * n_xy]
        for x in range(1, n_xy):
            total = total + rbuf[slot * n_xy + x]
        return total

    slots = [gathered(s) for s in range(len(lines))]
    r = slots[0]
    f = bottom(r, [slots[line_slot(o)] for o in near_offsets])
    fsend[...] = f
    copies4 = []
    for i, (a, b) in enumerate(lines):
        if i:
            copies4.append(send(fsend, fbuf.at[lines.index((-a % n_ta, -b % n_gz))], (a, b, 0)))
    pending += copies4
    fcol_re = jnp.sum(jnp.where(place, f[0:1], 0.0), axis=1, keepdims=True)
    fcol_im = jnp.sum(jnp.where(place, f[1:2], 0.0), axis=1, keepdims=True)
    psend[pl.ds(16, 16), :] = prolong(fcol_re, fcol_im)
    copies5 = [send(psend, pbuf.at[pl.ds(32 * i, 32)], offset) for i, offset in enumerate(hops)]
    pending += copies5
    for copy in copies4:
        copy.wait_recv()
    s = bottom(f, [fbuf[line_slot(o)] for o in near_offsets])

    rr, ri, fr, fi, sr, si = r[0:1], r[1:2], f[0:1], f[1:2], s[0:1], s[1:2]
    tsend[...] = jnp.concatenate(
        [
            fr * fr + fi * fi,
            sr * sr + si * si,
            fr * sr + fi * si,
            fr * si - fi * sr,
            fr * rr + fi * ri,
            fr * ri - fi * rr,
            sr * rr + si * ri,
            sr * ri - si * rr,
        ],
        axis=0,
    )
    copies6 = []
    for i, (a, b) in enumerate(plane):
        copies6.append(send(tsend, tbuf.at[i], (a, b, 0)))
    pending += copies6

    own_p = psend[...]
    lane32 = iota((32, 128), 1) & 31
    y_up = jnp.where(lane32 == 31, pltpu.roll(own_p, 31, 1), pltpu.roll(own_p, 127, 1))
    y_down = jnp.where(lane32 == 0, pltpu.roll(own_p, 97, 1), pltpu.roll(own_p, 1, 1))
    acc = [jnp.zeros((NV, 128), F32) for _ in range(4)]

    def add_direction(acc, d, v):
        acc = list(acc)
        for c in range(6):
            bre = mb[pl.ds(d * NV * 6 + c, NV, stride=6), :]
            bim = mb[pl.ds((9 + d) * NV * 6 + c, NV, stride=6), :]
            for image in range(2):
                vre = v[16 * image + c : 16 * image + c + 1]
                vim = v[16 * image + 8 + c : 16 * image + 9 + c]
                acc[2 * image] = acc[2 * image] + bre * vre - bim * vim
                acc[2 * image + 1] = acc[2 * image + 1] + bre * vim + bim * vre
        return acc

    acc = add_direction(acc, 0, own_p)
    acc = add_direction(acc, 7, y_up)
    acc = add_direction(acc, 8, y_down)
    for copy in copies5:
        copy.wait_recv()
    for i in range(6):
        acc = add_direction(acc, 1 + i, pbuf[pl.ds(32 * i, 32), :])
    lift = jnp.where(
        (iota((96, 32), 1) >> 3) == (iota((96, 32), 0).astype(F32) * (1.0 / NV) + 1e-3).astype(jnp.int32),
        1.0, 0.0,
    ).astype(F32)
    rows96 = iota((96, 32), 0)
    inner = rows96 - NV * (rows96.astype(F32) * (1.0 / NV) + 1e-3).astype(jnp.int32)
    lift = jnp.where((inner >> 2) == (iota((96, 32), 1) & 7), lift, 0.0)
    spread_p = dot(lift, own_p)
    keep = (iota((96, 128), 0) & 3) == (iota((96, 128), 1) >> 5)
    z = jnp.where(keep, spread_p, 0.0) * (1.0 - MIDDLE_DAMPING * MIDDLE_SHIFT)
    z = z - MIDDLE_DAMPING * jnp.concatenate(acc, axis=0)
    to_sites = jnp.where((li & 31) == (lj >> 2), 1.0, 0.0).astype(F32)
    u = dot(z, to_sites)
    same = jnp.where((li >> 2) == (lj >> 2), MIDDLE_DAMPING, 0.0).astype(F32)
    base = dot(sums, same)

    for copy in copies6:
        copy.wait_recv()
    total = tsend[...]
    for i in range(len(plane)):
        total = total + tbuf[i]
    total = jnp.sum(total, axis=1, keepdims=True)
    t = [total[i : i + 1] for i in range(8)]
    ff, ss, cre, cim, f_re, f_im, s_re, s_im = t
    det = ff * ss - cre * cre - cim * cim
    c1r = (ss * f_re - (cre * s_re - cim * s_im)) / det
    c1i = (ss * f_im - (cre * s_im + cim * s_re)) / det
    c2r = (ff * s_re - (cre * f_re + cim * f_im)) / det
    c2i = (ff * s_im - (cre * f_im - cim * f_re)) / det
    ur_re, ur_im, uf_re, uf_im = (u[NV * q : NV * (q + 1)] for q in range(4))
    up_re = base[:NV] + c1r * ur_re - c1i * ur_im + c2r * uf_re - c2i * uf_im
    up_im = base[NV:] + c1r * ur_im + c1i * ur_re + c2r * uf_im + c2i * uf_re
    up_re = up_re.astype(BF16).astype(F32)
    up_im = up_im.astype(BF16).astype(F32)
    out_re = jnp.zeros((NSC, 128), F32)
    out_im = jnp.zeros((NSC, 128), F32)
    for k in range(NV):
        fre = fine32[pl.ds(k * NSC, NSC), :]
        fim = fine32[pl.ds((NV + k) * NSC, NSC), :]
        a, b = up_re[k : k + 1], up_im[k : k + 1]
        out_re = out_re + fre * a - fim * b
        out_im = out_im + fre * b + fim * a
    order = [c * 4 + spin for spin in range(4) for c in range(NC)]
    correction = jnp.concatenate(
        [part[i : i + 1] for part in (out_re, out_im) for i in order], axis=0
    )
    result_ref[pl.ds(0, 24), :] = second_value + correction
    for copy in pending:
        copy.wait_send()


def part_outputs(both, solution_ref, residual_ref):
    solution_ref[...] = both[pl.ds(0, 24), :]
    residual_ref[...] = both[pl.ds(24, 24), :]


def shards(sizes, source_field, gauge_links, fine_vectors, middle_blocks, middle_vectors, bottom_blocks):
    lines, hops, plane, spread, peers = plan(sizes)
    n_xy = sizes[2]
    chunks = n_xy * NV * NV // 128
    width = -(-n_xy * NV // 128) * 128
    copies = 3 * len(hops) + len(spread) + len(lines) - 1 + len(plane)
    vmem = pl.BlockSpec(memory_space=pltpu.VMEM)
    hbm = pl.BlockSpec(memory_space=pl.ANY)
    out = jax.ShapeDtypeStruct((24, 128), F32)
    both = pl.pallas_call(
        functools.partial(kernel, sizes),
        out_shape=jax.ShapeDtypeStruct((48, 128), F32),
        in_specs=[vmem, hbm, hbm, hbm, hbm, hbm],
        out_specs=vmem,
        scratch_shapes=[
            pltpu.VMEM((144, 128), F32),
            pltpu.VMEM((2 * NV * NC, 4, 128), BF16),
            pltpu.VMEM((2 * 9 * NV * 6, 128), F32),
            pltpu.VMEM((2 * NV * 6, 128), F32),
            pltpu.VMEM(((15 * chunks + 7) // 8 * 8, 128), F32),
            pltpu.VMEM((2 * NV * NSC, 128), F32),
            pltpu.VMEM((192, 128), F32),
            pltpu.VMEM((192, 128), F32),
            pltpu.VMEM((24, 128), F32),
            pltpu.VMEM((width, n_xy * NV * NV), BF16),
            pltpu.VMEM((width, n_xy * NV * NV), BF16),
            pltpu.VMEM((8, width), F32),
            pltpu.VMEM((len(lines) * n_xy, 8, width), F32),
            pltpu.VMEM((8, width), F32),
            pltpu.VMEM((len(lines), 8, width), F32),
            pltpu.VMEM((32, 128), F32),
            pltpu.VMEM((6 * 32, 128), F32),
            pltpu.VMEM((8, width), F32),
            pltpu.VMEM((len(plane), 8, width), F32),
            pltpu.SemaphoreType.DMA((5,)),
            pltpu.SemaphoreType.DMA((copies,)),
            pltpu.SemaphoreType.DMA((copies,)),
        ],
        compiler_params=pltpu.CompilerParams(
            collective_id=0, has_side_effects=True, vmem_limit_bytes=60 * 1024 * 1024
        ),
    )(
        source_field.reshape(24, 128),
        gauge_links.reshape(144, 128),
        jnp.swapaxes(fine_vectors, 2, 3).reshape(2 * NV * NC, 4, 128),
        middle_blocks.reshape(-1, 128),
        middle_vectors.reshape(-1, 128),
        bottom_blocks.reshape(-1, 1, 128),
    )
    results = pl.pallas_call(
        part_outputs, out_shape=(out, out), in_specs=[vmem], out_specs=(vmem, vmem)
    )(both)
    return tuple(x.reshape(source_field.shape) for x in results)


def solution(mesh):
    sizes = tuple(mesh.shape[a] for a in AXES)
    return jax.shard_map(
        functools.partial(shards, sizes),
        mesh=mesh,
        in_specs=(
            P(None, None, None, "ta", "gz", "xy", None),
            P(None, None, None, None, "ta", "gz", "xy", None),
            P(None, None, None, None, "ta", "gz", "xy", None),
            P(None, None, None, "ta", "gz", "xy", None),
            P(None, None, "ta", "gz", "xy", None),
            P(None, None, "ta", "gz", None),
        ),
        out_specs=(
            P(None, None, None, "ta", "gz", "xy", None),
            P(None, None, None, "ta", "gz", "xy", None),
        ),
        check_vma=False,
    )
```

```python
import functools

import jax
import jax.numpy as jnp
from jax import lax
from jax.experimental import pallas as pl
from jax.experimental.pallas import tpu as pltpu
from jax.sharding import PartitionSpec as P

BY = 4
NV = 24
NC = 3
NSC = 12

DIAGONAL = 4.0 + 0.1
TWIST = 0.1
DENOMINATOR = DIAGONAL * DIAGONAL + TWIST * TWIST
FINE_DAMPING = 0.8
MIDDLE_DAMPING = 0.4
MIDDLE_SHIFT = 2.0
BOTTOM_SHIFT = 2.0
MESH = pl.DeviceIdType.MESH
F32 = jnp.float32
BF16 = jnp.bfloat16
AXES = ("ta", "gz", "xy")


def plan(sizes):
    n_ta, n_gz, n_xy = sizes
    lines = []
    for offset in ((0, 0), (1, 0), (-1, 0), (0, 1), (0, -1)):
        reduced = (offset[0] % n_ta, offset[1] % n_gz)
        if reduced not in lines:
            lines.append(reduced)
    wide = list(lines)
    for a in lines:
        for b in lines:
            both = ((a[0] + b[0]) % n_ta, (a[1] + b[1]) % n_gz)
            if both not in wide:
                wide.append(both)
    hops = []
    for axis in range(3):
        for step in (1, -1):
            offset = [0, 0, 0]
            offset[axis] = -step % sizes[axis]
            hops.append(tuple(offset))
    plane = [(a, b) for a in range(n_ta) for b in range(n_gz) if (a, b) != (0, 0)]
    spread = [(a, b, x) for a, b in wide for x in range(n_xy) if (a, b, x) != (0, 0, 0)]
    def distance(offset):
        return sum(min(o, n - o) for o, n in zip(offset, sizes))

    far = [o for o in [(a, b, 0) for a, b in plane] + spread if distance(o) > 3]
    peers = []
    for offset in hops + far:
        back = tuple(-o % n for o, n in zip(offset, sizes))
        for one in (offset, back):
            if one not in peers:
                peers.append(one)
    return lines, wide, hops, plane, spread, peers


def dot(a, b, dims=((1,), (0,))):
    return lax.dot_general(
        a, b, (dims, ((), ())), precision=lax.Precision.HIGHEST, preferred_element_type=F32
    )


def split_dot(a, b, dims):
    high = a.astype(BF16)
    low = (a - high.astype(F32)).astype(BF16)
    rows = a.shape[0]
    both = lax.dot_general(
        jnp.concatenate([high, low], axis=0), b, (dims, ((), ())), preferred_element_type=F32
    )
    return both[:rows] + both[rows:]


def iota(shape, dim):
    return lax.broadcasted_iota(jnp.int32, shape, dim)


def hopping(load, gauge):
    row = iota((8, 128), 0)
    odd = (row & 1) == 1
    m = row >> 1
    near = m < 2
    eps = jnp.where(odd, 1.0, -1.0).astype(F32)

    def phase(values):
        re = jnp.zeros((8, 128), F32)
        im = jnp.zeros((8, 128), F32)
        for i, (a, b) in enumerate(values):
            re = jnp.where(m == i, a, re)
            im = jnp.where(m == i, b, im)
        return re * eps, im * eps

    up0 = phase(((1.0, 0.0), (0.0, 1.0), (0.0, 1.0), (-1.0, 0.0)))
    up1 = phase(((1.0, 0.0), (0.0, -1.0), (0.0, 1.0), (1.0, 0.0)))
    low2 = phase(((1.0, 0.0), (0.0, -1.0), (0.0, -1.0), (1.0, 0.0)))
    low3 = phase(((1.0, 0.0), (0.0, 1.0), (0.0, -1.0), (-1.0, 0.0)))

    def times(c, re, im):
        return c[0] * re - c[1] * im, c[0] * im + c[1] * re

    half = {}
    for color in range(NC):
        v = [load(spin, color) for spin in range(4)]
        for spin, c in ((0, up0), (1, up1)):
            first, other = (v[2], v[3]) if spin == 0 else (v[3], v[2])
            re = jnp.where(near, first[0], other[0])
            im = jnp.where(near, first[1], other[1])
            re, im = times(c, re, im)
            half[spin, color] = (v[spin][0] + re, v[spin][1] + im)
    out = {}
    for c in range(NC):
        acc = {0: None, 1: None}
        for k in range(NC):
            ure = gauge[pl.ds(c * 3 + k, 8, stride=9), :]
            uim = gauge[pl.ds(72 + c * 3 + k, 8, stride=9), :]
            for spin in range(2):
                hre, him = half[spin, k]
                re = ure * hre - uim * him
                im = ure * him + uim * hre
                acc[spin] = (re, im) if acc[spin] is None else (acc[spin][0] + re, acc[spin][1] + im)
        w0, w1 = acc[0], acc[1]
        out[0, c] = w0
        out[1, c] = w1
        for spin, coef in ((2, low2), (3, low3)):
            first, other = (w0, w1) if spin == 2 else (w1, w0)
            re = jnp.where(near, first[0], other[0])
            im = jnp.where(near, first[1], other[1])
            out[spin, c] = times(coef, re, im)
    rows = [
        jnp.sum(out[spin, c][part], axis=0, keepdims=True)
        for part in range(2)
        for spin in range(4)
        for c in range(NC)
    ]
    return jnp.concatenate(rows, axis=0)


def signs_of():
    row = iota((24, 128), 0)
    inner = jnp.where(row >= NSC, row - NSC, row)
    return jnp.where(inner < 6, 1.0, -1.0).astype(F32), row < NSC


def swap(v):
    return jnp.concatenate([v[NSC:], v[:NSC]], axis=0)


def twisted(v):
    g5, real = signs_of()
    return DIAGONAL * v + TWIST * jnp.where(real, -g5, g5) * swap(v)


def precondition(v):
    g5, real = signs_of()
    return (DIAGONAL * v + TWIST * jnp.where(real, g5, -g5) * swap(v)) * (1.0 / DENOMINATOR)


def kernel(
    sizes, source_hbm, gauge_hbm, fine_hbm, mb_hbm, mv_hbm, bb_hbm,
    result_ref,
    source, gauge, fine, mb, mv, bb, fine32, near1, near2, second, expand, reduce,
    rsend, rbuf, psend, pbuf, tsend, tbuf,
    local_sem, send_sem, recv_sem,
):
    n_ta, n_gz, n_xy = sizes
    lines, wide, hops, plane, spread, peers = plan(sizes)
    me = tuple(lax.axis_index(a) for a in AXES)
    chunks = n_xy * NV * NV // 128
    width = rsend.shape[1]

    def device(offset):
        return tuple(lax.rem(m + o, n) for m, o, n in zip(me, offset, sizes))

    loads = [
        pltpu.make_async_copy(gauge_hbm, gauge, local_sem.at[0]),
        pltpu.make_async_copy(mb_hbm, mb, local_sem.at[1]),
        pltpu.make_async_copy(mv_hbm, mv, local_sem.at[2]),
        pltpu.make_async_copy(bb_hbm.at[:, 0, :], bb.at[0, pl.ds(0, 14 * chunks)], local_sem.at[3]),
    ]
    fine_copy = pltpu.make_async_copy(fine_hbm, fine, local_sem.at[4])
    source_copy = pltpu.make_async_copy(source_hbm, source, local_sem.at[5])
    loads = [source_copy, loads[0], loads[3], loads[2], loads[1], fine_copy]
    barrier = pltpu.get_barrier_semaphore()
    for offset in peers:
        pl.semaphore_signal(barrier, inc=1, device_id=device(offset), device_id_type=MESH)
    for load in loads:
        load.start()

    for i in range(len(lines)):
        bb[i, pl.ds(14 * chunks, bb.shape[1] - 14 * chunks), :] = jnp.zeros(
            (bb.shape[1] - 14 * chunks, 128), F32
        )
    count = [0]

    def send(src, dst, offset):
        copy = pltpu.make_async_remote_copy(
            src_ref=src, dst_ref=dst, send_sem=send_sem.at[count[0]],
            recv_sem=recv_sem.at[count[0]], device_id=device(offset), device_id_type=MESH,
        )
        count[0] += 1
        copy.start()
        return copy

    source_copy.wait()
    pl.semaphore_wait(barrier, len(peers))
    pending = []

    def halo(src, buf):
        return [send(src, buf.at[pl.ds(24 * i, 24)], offset) for i, offset in enumerate(hops)]

    def fill_y(v, buf):
        buf[pl.ds(24 * 6, 24), :] = pltpu.roll(v, 127, 1)
        buf[pl.ds(24 * 7, 24), :] = pltpu.roll(v, 1, 1)

    copies1 = halo(source, near1)
    pending += copies1
    loads[2].wait()

    def bulk(first_line, last_line):
        return [
            send(
                bb.at[0, pl.ds(0, 14 * chunks)],
                bb.at[lines.index((-a % n_ta, -b % n_gz)), pl.ds(0, 14 * chunks)],
                (a, b, 0),
            )
            for a, b in lines[first_line:last_line]
        ]

    bulks = bulk(1, 2)
    src = source[...]
    fill_y(src, near1)
    first = FINE_DAMPING * precondition(src)

    cols = n_xy * NV * NV
    n = iota((1, cols), 1).astype(F32)
    xs = jnp.floor((n + 0.5) * (1.0 / (NV * NV)))
    js = jnp.floor((n - xs * (NV * NV) + 0.5) * (1.0 / NV))
    ks = n - xs * (NV * NV) - js * NV
    lane = iota((width, cols), 0).astype(F32)
    expand[...] = jnp.where(lane == xs * NV + ks, 1.0, 0.0).astype(BF16)
    reduce[...] = jnp.where(lane == xs * NV + js, 1.0, 0.0).astype(BF16)
    fine_copy.wait()
    fine32[...] = fine[...].astype(F32).reshape(2 * NV * NSC, 128)

    def loader(buf, scaled):
        def load(spin, color):
            i = spin * NC + color
            re = buf[pl.ds(i, 8, stride=24), :]
            im = buf[pl.ds(NSC + i, 8, stride=24), :]
            if not scaled:
                return re, im
            a = FINE_DAMPING * DIAGONAL / DENOMINATOR
            b = FINE_DAMPING * TWIST / DENOMINATOR * (1.0 if spin < 2 else -1.0)
            return a * re + b * im, a * im - b * re
        return load

    loads[1].wait()
    for copy in copies1:
        copy.wait_recv()
    hop = hopping(loader(near1, True), gauge)
    second_value = first + FINE_DAMPING * precondition(src - (twisted(first) - 0.5 * hop))
    second[...] = second_value
    copies2 = halo(second, near2)
    pending += copies2
    bulks += bulk(2, len(lines))
    pending += bulks
    fill_y(second_value, near2)
    loads[3].wait()
    loads[4].wait()
    for copy in copies2:
        copy.wait_recv()
    hop = hopping(loader(near2, False), gauge)
    smoothed = src - (twisted(second_value) - 0.5 * hop)
    result_ref[pl.ds(24, 24), :] = smoothed
    low = smoothed.astype(BF16).astype(F32)

    mre = jnp.zeros((NV, 128), F32)
    mim = jnp.zeros((NV, 128), F32)
    for i in range(NSC):
        fre = fine32[pl.ds(i, NV, stride=NSC), :]
        fim = fine32[pl.ds(NV * NSC + i, NV, stride=NSC), :]
        at = i % 4 * NC + i // 4
        rre, rim = low[at : at + 1], low[NSC + at : NSC + at + 1]
        mre = mre + fre * rre + fim * rim
        mim = mim + fre * rim - fim * rre
    sums = jnp.concatenate([mre, mim], axis=0)
    li = iota((128, 128), 0)
    lj = iota((128, 128), 1)
    group = jnp.where((li >> 2) == (lj & 31), 1.0, 0.0).astype(F32)
    rep = dot(sums, group)
    own_group = ((iota((48, 128), 0) & 3) == (iota((48, 128), 1) >> 5))
    masked = jnp.where(own_group, rep, 0.0)
    gather = jnp.where(iota((16, 48), 0) == (iota((16, 48), 1) >> 2), 1.0, 0.0).astype(F32)
    mr = dot(gather, masked)

    are = jnp.zeros((NV, 128), F32)
    aim = jnp.zeros((NV, 128), F32)
    for c in range(6):
        vre = mv[pl.ds(c, NV, stride=6), :]
        vim = mv[pl.ds(NV * 6 + c, NV, stride=6), :]
        rre, rim = mr[c : c + 1], mr[6 + c : 7 + c]
        are = are + vre * rre + vim * rim
        aim = aim + vre * rim - vim * rre
    rcol_re = jnp.sum(are, axis=1, keepdims=True)
    rcol_im = jnp.sum(aim, axis=1, keepdims=True)
    place = iota((NV, width), 1) == me[2] * NV + iota((NV, width), 0)
    own_re = jnp.sum(jnp.where(place, rcol_re, 0.0), axis=0, keepdims=True)
    own_im = jnp.sum(jnp.where(place, rcol_im, 0.0), axis=0, keepdims=True)
    tile_row = iota((8, width), 0)

    def pair_tile(re, im):
        return jnp.where(tile_row == 0, re, jnp.where(tile_row == 1, im, 0.0))

    own_tile = pair_tile(own_re, own_im)
    rsend[...] = own_tile
    copies3 = []
    for a, b, x in spread:
        slot = wide.index((-a % n_ta, -b % n_gz))
        copies3.append(send(rsend, rbuf.at[slot * n_xy + x], (a, b, x)))
    pending += copies3

    def prolong(re, im):
        re = jnp.broadcast_to(re, (NV, 128))
        im = jnp.broadcast_to(im, (NV, 128))
        rows_re, rows_im = [], []
        for c in range(6):
            vre = mv[pl.ds(c, NV, stride=6), :]
            vim = mv[pl.ds(NV * 6 + c, NV, stride=6), :]
            rows_re.append(jnp.sum(vre * re - vim * im, axis=0, keepdims=True))
            rows_im.append(jnp.sum(vre * im + vim * re, axis=0, keepdims=True))
        zero = jnp.zeros((2, 128), F32)
        return jnp.concatenate(rows_re + [zero] + rows_im + [zero], axis=0)

    psend[pl.ds(0, 16), :] = prolong(rcol_re, rcol_im)

    for copy in copies3:
        copy.wait_recv()

    def line_slot(offset):
        return wide.index((offset[0] % n_ta, offset[1] % n_gz))

    near_offsets = ((1, 0), (-1, 0), (0, 1), (0, -1))
    length = n_xy * NV

    def turn(v, shift):
        lanes = iota(v.shape, 1)
        if shift > 0:
            inside, wrapped = lanes < length - shift, length - shift
            one, two = pltpu.roll(v, width - shift, 1), pltpu.roll(v, wrapped, 1)
        else:
            inside = lanes >= -shift
            one, two = pltpu.roll(v, -shift, 1), pltpu.roll(v, width - (length + shift), 1)
        return jnp.where(lanes < length, jnp.where(inside, one, two), 0.0)

    def bottom(systems):
        zero = jnp.zeros((1, width), F32)
        stacks = []
        for own, others, _ in systems:
            near = [own] + others + [turn(own, NV), turn(own, -NV)]
            stacks += [v[0:1] for v in near] + [zero] + [v[1:2] for v in near] + [zero]
        broad = split_dot(jnp.concatenate(stacks, axis=0), expand[...], ((1,), (0,)))
        prods = []
        for q, (_, _, line) in enumerate(systems):
            parts = []
            for c in range(chunks):
                bre = bb[line, pl.ds(c, 8, stride=chunks), :]
                bim = bb[line, pl.ds(7 * chunks + c, 8, stride=chunks), :]
                vre = broad[16 * q : 16 * q + 8, c * 128 : (c + 1) * 128]
                vim = broad[16 * q + 8 : 16 * q + 16, c * 128 : (c + 1) * 128]
                parts.append(
                    jnp.concatenate([bre * vre - bim * vim, bre * vim + bim * vre], axis=0)
                )
            prods.append(jnp.concatenate(parts, axis=1))
        short = split_dot(jnp.concatenate(prods, axis=0), reduce[...], ((1,), (1,)))
        results = []
        for q, (own, _, _) in enumerate(systems):
            re = jnp.sum(short[16 * q : 16 * q + 8], axis=0, keepdims=True)
            im = jnp.sum(short[16 * q + 8 : 16 * q + 16], axis=0, keepdims=True)
            results.append(pair_tile(re, im) + BOTTOM_SHIFT * own)
        return results

    def gathered(slot):
        total = own_tile if slot == 0 else rbuf[slot * n_xy]
        for x in range(1, n_xy):
            total = total + rbuf[slot * n_xy + x]
        return total

    slots = [gathered(s) for s in range(len(wide))]
    r = slots[0]
    for copy in bulks:
        copy.wait_recv()
    systems = []
    for i, (a, b) in enumerate(lines):
        systems.append((slots[i], [slots[line_slot((a + p, b + q))] for p, q in near_offsets], i))
    images = bottom(systems)
    f = images[0]
    fcol_re = jnp.sum(jnp.where(place, f[0:1], 0.0), axis=1, keepdims=True)
    fcol_im = jnp.sum(jnp.where(place, f[1:2], 0.0), axis=1, keepdims=True)
    psend[pl.ds(16, 16), :] = prolong(fcol_re, fcol_im)
    copies5 = [send(psend, pbuf.at[pl.ds(32 * i, 32)], offset) for i, offset in enumerate(hops)]
    pending += copies5
    s = bottom([(f, [images[line_slot(o)] for o in near_offsets], 0)])[0]

    rr, ri, fr, fi, sr, si = r[0:1], r[1:2], f[0:1], f[1:2], s[0:1], s[1:2]
    tsend[...] = jnp.concatenate(
        [
            fr * fr + fi * fi,
            sr * sr + si * si,
            fr * sr + fi * si,
            fr * si - fi * sr,
            fr * rr + fi * ri,
            fr * ri - fi * rr,
            sr * rr + si * ri,
            sr * ri - si * rr,
        ],
        axis=0,
    )
    copies6 = []
    for i, (a, b) in enumerate(plane):
        copies6.append(send(tsend, tbuf.at[i], (a, b, 0)))
    pending += copies6

    own_p = psend[...]
    lane32 = iota((32, 128), 1) & 31
    y_up = jnp.where(lane32 == 31, pltpu.roll(own_p, 31, 1), pltpu.roll(own_p, 127, 1))
    y_down = jnp.where(lane32 == 0, pltpu.roll(own_p, 97, 1), pltpu.roll(own_p, 1, 1))
    acc = [jnp.zeros((NV, 128), F32) for _ in range(4)]

    def add_direction(acc, d, v):
        acc = list(acc)
        for c in range(6):
            bre = mb[pl.ds(d * NV * 6 + c, NV, stride=6), :]
            bim = mb[pl.ds((9 + d) * NV * 6 + c, NV, stride=6), :]
            for image in range(2):
                vre = v[16 * image + c : 16 * image + c + 1]
                vim = v[16 * image + 8 + c : 16 * image + 9 + c]
                acc[2 * image] = acc[2 * image] + bre * vre - bim * vim
                acc[2 * image + 1] = acc[2 * image + 1] + bre * vim + bim * vre
        return acc

    acc = add_direction(acc, 0, own_p)
    acc = add_direction(acc, 7, y_up)
    acc = add_direction(acc, 8, y_down)
    for copy in copies5:
        copy.wait_recv()
    for i in range(6):
        acc = add_direction(acc, 1 + i, pbuf[pl.ds(32 * i, 32), :])
    lift = jnp.where(
        (iota((96, 32), 1) >> 3) == (iota((96, 32), 0).astype(F32) * (1.0 / NV) + 1e-3).astype(jnp.int32),
        1.0, 0.0,
    ).astype(F32)
    rows96 = iota((96, 32), 0)
    inner = rows96 - NV * (rows96.astype(F32) * (1.0 / NV) + 1e-3).astype(jnp.int32)
    lift = jnp.where((inner >> 2) == (iota((96, 32), 1) & 7), lift, 0.0)
    spread_p = dot(lift, own_p)
    keep = (iota((96, 128), 0) & 3) == (iota((96, 128), 1) >> 5)
    z = jnp.where(keep, spread_p, 0.0) * (1.0 - MIDDLE_DAMPING * MIDDLE_SHIFT)
    z = z - MIDDLE_DAMPING * jnp.concatenate(acc, axis=0)
    to_sites = jnp.where((li & 31) == (lj >> 2), 1.0, 0.0).astype(F32)
    u = dot(z, to_sites)
    same = jnp.where((li >> 2) == (lj >> 2), MIDDLE_DAMPING, 0.0).astype(F32)
    base = dot(sums, same)

    for copy in copies6:
        copy.wait_recv()
    total = tsend[...]
    for i in range(len(plane)):
        total = total + tbuf[i]
    total = jnp.sum(total, axis=1, keepdims=True)
    t = [total[i : i + 1] for i in range(8)]
    ff, ss, cre, cim, f_re, f_im, s_re, s_im = t
    det = ff * ss - cre * cre - cim * cim
    c1r = (ss * f_re - (cre * s_re - cim * s_im)) / det
    c1i = (ss * f_im - (cre * s_im + cim * s_re)) / det
    c2r = (ff * s_re - (cre * f_re + cim * f_im)) / det
    c2i = (ff * s_im - (cre * f_im - cim * f_re)) / det
    ur_re, ur_im, uf_re, uf_im = (u[NV * q : NV * (q + 1)] for q in range(4))
    up_re = base[:NV] + c1r * ur_re - c1i * ur_im + c2r * uf_re - c2i * uf_im
    up_im = base[NV:] + c1r * ur_im + c1i * ur_re + c2r * uf_im + c2i * uf_re
    up_re = up_re.astype(BF16).astype(F32)
    up_im = up_im.astype(BF16).astype(F32)
    out_re = jnp.zeros((NSC, 128), F32)
    out_im = jnp.zeros((NSC, 128), F32)
    for k in range(NV):
        fre = fine32[pl.ds(k * NSC, NSC), :]
        fim = fine32[pl.ds((NV + k) * NSC, NSC), :]
        a, b = up_re[k : k + 1], up_im[k : k + 1]
        out_re = out_re + fre * a - fim * b
        out_im = out_im + fre * b + fim * a
    order = [c * 4 + spin for spin in range(4) for c in range(NC)]
    correction = jnp.concatenate(
        [part[i : i + 1] for part in (out_re, out_im) for i in order], axis=0
    )
    result_ref[pl.ds(0, 24), :] = second_value + correction
    for copy in pending:
        copy.wait_send()


def part_outputs(both, solution_ref, residual_ref):
    solution_ref[...] = both[pl.ds(0, 24), :]
    residual_ref[...] = both[pl.ds(24, 24), :]


def shards(sizes, source_field, gauge_links, fine_vectors, middle_blocks, middle_vectors, bottom_blocks):
    lines, wide, hops, plane, spread, peers = plan(sizes)
    n_xy = sizes[2]
    chunks = n_xy * NV * NV // 128
    width = -(-n_xy * NV // 128) * 128
    copies = 3 * len(hops) + len(spread) + len(lines) - 1 + len(plane)
    vmem = pl.BlockSpec(memory_space=pltpu.VMEM)
    hbm = pl.BlockSpec(memory_space=pl.ANY)
    out = jax.ShapeDtypeStruct((24, 128), F32)
    both = pl.pallas_call(
        functools.partial(kernel, sizes),
        out_shape=jax.ShapeDtypeStruct((48, 128), F32),
        in_specs=[hbm] * 6,
        out_specs=vmem,
        scratch_shapes=[
            pltpu.VMEM((24, 128), F32),
            pltpu.VMEM((144, 128), F32),
            pltpu.VMEM((2 * NV * NC, 4, 128), BF16),
            pltpu.VMEM((2 * 9 * NV * 6, 128), F32),
            pltpu.VMEM((2 * NV * 6, 128), F32),
            pltpu.VMEM((len(lines), (15 * chunks + 7) // 8 * 8, 128), F32),
            pltpu.VMEM((2 * NV * NSC, 128), F32),
            pltpu.VMEM((192, 128), F32),
            pltpu.VMEM((192, 128), F32),
            pltpu.VMEM((24, 128), F32),
            pltpu.VMEM((width, n_xy * NV * NV), BF16),
            pltpu.VMEM((width, n_xy * NV * NV), BF16),
            pltpu.VMEM((8, width), F32),
            pltpu.VMEM((len(wide) * n_xy, 8, width), F32),
            pltpu.VMEM((32, 128), F32),
            pltpu.VMEM((6 * 32, 128), F32),
            pltpu.VMEM((8, width), F32),
            pltpu.VMEM((len(plane), 8, width), F32),
            pltpu.SemaphoreType.DMA((6,)),
            pltpu.SemaphoreType.DMA((copies,)),
            pltpu.SemaphoreType.DMA((copies,)),
        ],
        compiler_params=pltpu.CompilerParams(
            collective_id=0, has_side_effects=True, vmem_limit_bytes=60 * 1024 * 1024
        ),
    )(
        source_field.reshape(24, 128),
        gauge_links.reshape(144, 128),
        jnp.swapaxes(fine_vectors, 2, 3).reshape(2 * NV * NC, 4, 128),
        middle_blocks.reshape(-1, 128),
        middle_vectors.reshape(-1, 128),
        bottom_blocks.reshape(-1, 1, 128),
    )
    results = pl.pallas_call(
        part_outputs, out_shape=(out, out), in_specs=[vmem], out_specs=(vmem, vmem)
    )(both)
    return tuple(x.reshape(source_field.shape) for x in results)


def solution(mesh):
    sizes = tuple(mesh.shape[a] for a in AXES)
    return jax.shard_map(
        functools.partial(shards, sizes),
        mesh=mesh,
        in_specs=(
            P(None, None, None, "ta", "gz", "xy", None),
            P(None, None, None, None, "ta", "gz", "xy", None),
            P(None, None, None, None, "ta", "gz", "xy", None),
            P(None, None, None, "ta", "gz", "xy", None),
            P(None, None, "ta", "gz", "xy", None),
            P(None, None, "ta", "gz", None),
        ),
        out_specs=(
            P(None, None, None, "ta", "gz", "xy", None),
            P(None, None, None, "ta", "gz", "xy", None),
        ),
        check_vma=False,
    )
```
